256 devices in a mesh: dp: 32 (over y, z), mp: 8 (over x, core).
Axes of the slice: x: 4, y: 4, z: 8, core: 2. Of those that a mesh axis runs over, the one named last changes fastest.
Arguments:
- queries: bfloat16 [1024, 64, 16, 128], P('dp', 'mp'), may hold values from -5 to 5
- draft_kv: bfloat16 [1024, 2, 8, 16, 128], P('dp', None, 'mp'), may hold values from -5 to 5
- kv_pool: bfloat16 [16384, 2, 8, 16, 128], P('dp', None, 'mp'), may hold values from -5 to 5
- block_dest: int32 [16384], P('dp'), may hold values from -1 to 31, as said below
- block_table: int32 [1024, 32], P('dp'), may hold values from 0 to 1023, as said below
- context_len: int32 [1024], P('dp'), may hold values from 0 to 512
- draft_len: int32 [1024], P('dp'), may hold values from 2 to 16
- accept_mask: int32 [1024, 16], P('dp'), may hold values 0 or 1
- out_weight: bfloat16 [8192, 4096], P('mp'), may hold values from -0.5 to 0.5
- residual: bfloat16 [16384, 4096], P('dp'), may hold values from -80 to 80
- norm_gain: float32 [4096], P('mp'), may hold values from 0.1 to 1.9
Outputs:
- normed: bfloat16 [16384, 4096], P('dp', 'mp')
The draws below stay inside these ranges and needn't reach their ends.
Inputs may be any that keep to these rules, and one draw needn't show every extreme that they name: Pool block b belongs to rank b // 512 and goes to rank block_dest[b]; -1 marks a free block. A rank sends at most 32 blocks to one rank, and some rank receives exactly 32 blocks from every rank. `block_table`: entry e of request r is read where e * 16 < context_len[r]. Such an entry names slot s * 32 + k of the blocks received by rank r // 32, one that holds a block (the k-th, in pool order, that rank s sends there); the entries read on one rank name distinct slots, and every received block is named by one of them.
All inputs are finite; a program needn't handle non-finite values. No bound on the sum of `accept_mask` on one device may be relied on, other than what follows from the above.
Results may differ from the reference program's by a relative error of at most 0.011.
Values may be sent and summed in bfloat16 or wider, within the bound.
No kernel may reach another device: no remote copies, remote signals or barrier semaphores. Data moves between devices by JAX's collectives and lax.ppermute only.
A program may use at most 192 MiB of HBM per device.

```python
import math
import jax
import jax.numpy as jnp
from jax import lax

QH = 64
KVH = 8
HD = 128
DWIN = 4096
P_SIZE = 16
W = 16
MAXB = 32
REQ = 32
NB_DEV = 512
SLOTS = 32
REQUESTS = 1024
POOL = 16384
ROWS = 16384
N_DP = 32
N_MP = 8


def routing_plan(key):
    rank_count = N_DP
    keys = jax.random.split(jax.random.fold_in(key, 9173), 7)
    ranking = jax.random.permutation(keys[0], rank_count)
    heavy = jnp.zeros((rank_count,), jnp.int32).at[ranking[:rank_count // 4]].set(1)
    ceiling = jnp.where(heavy == 1, SLOTS, SLOTS // 3)
    counts = jax.random.randint(keys[1], (rank_count, rank_count), 0, ceiling[None, :] + 1, dtype=jnp.int32)
    counts = counts.at[:, ranking[0]].set(SLOTS)
    ends = jnp.cumsum(counts, axis=1, dtype=jnp.int32)
    positions = jnp.arange(NB_DEV, dtype=jnp.int32)
    target_rank = jnp.sum((positions[None, :, None] >= ends[:, None, :]).astype(jnp.int32), axis=2, dtype=jnp.int32)
    target_rank = jnp.where(target_rank >= rank_count, -1, target_rank)
    shuffles = jax.vmap(lambda sub_key: jax.random.permutation(sub_key, NB_DEV))(jax.random.split(keys[2], rank_count))
    destinations = jnp.take_along_axis(target_rank, shuffles, axis=1)
    arrived_count = jnp.sum(counts, axis=0, dtype=jnp.int32)
    slot_ids = jnp.arange(rank_count * SLOTS, dtype=jnp.int32)
    filled = ((slot_ids % SLOTS)[None, :] < counts[slot_ids // SLOTS, :].T).astype(jnp.int32)
    noise = jax.vmap(lambda sub_key: jax.random.permutation(sub_key, rank_count * SLOTS))(jax.random.split(keys[3], rank_count))
    ordering = jnp.argsort((1 - filled) * (rank_count * SLOTS) + noise, axis=1, stable=True)
    base_count = arrived_count // REQ
    extra_count = arrived_count % REQ
    per_request = base_count[:, None] + (jnp.arange(REQ, dtype=jnp.int32)[None, :] < extra_count[:, None]).astype(jnp.int32)
    first_half = per_request[:, 0::2]
    second_half = per_request[:, 1::2]
    headroom = jnp.minimum(second_half, MAXB - first_half)
    shifted = jax.random.randint(keys[4], first_half.shape, 0, headroom + 1, dtype=jnp.int32)
    per_request = jnp.stack([first_half + shifted, second_half - shifted], axis=2).reshape(rank_count, REQ)
    request_order = jax.vmap(lambda sub_key: jax.random.permutation(sub_key, REQ))(jax.random.split(keys[5], rank_count))
    per_request = jnp.take_along_axis(per_request, request_order, axis=1)
    starts = jnp.cumsum(per_request, axis=1, dtype=jnp.int32) - per_request
    entries = jnp.arange(MAXB, dtype=jnp.int32)
    position_index = jnp.minimum(starts[:, :, None] + entries[None, None, :], rank_count * SLOTS - 1)
    picked = jnp.take_along_axis(ordering, position_index.reshape(rank_count, REQ * MAXB), axis=1).reshape(rank_count, REQ, MAXB)
    table = jnp.where(entries[None, None, :] < per_request[:, :, None], picked, 0)
    lower = jnp.where(per_request > 0, (per_request - 1) * P_SIZE + 1, 0)
    upper = per_request * P_SIZE
    context = jax.random.randint(keys[6], per_request.shape, lower, upper + 1, dtype=jnp.int32)
    return (destinations.reshape(-1).astype(jnp.int32), table.reshape(rank_count * REQ, MAXB).astype(jnp.int32), context.reshape(-1).astype(jnp.int32))


def draw_block_dest(key, part):
    return routing_plan(key)[0]


def draw_block_table(key, part):
    return routing_plan(key)[1]


def draw_context_len(key, part):
    return routing_plan(key)[2]


def draw_queries(key, part):
    shape = (REQUESTS, QH, W, HD)
    base_key = jax.random.fold_in(key, 31)
    values = jnp.clip(jax.random.normal(base_key, shape, jnp.float32), -5.0, 5.0)
    return values.astype(jnp.bfloat16)


def draw_draft_kv(key, part):
    shape = (REQUESTS, 2, KVH, W, HD)
    base_key = jax.random.fold_in(key, 57)
    values = jnp.clip(jax.random.normal(base_key, shape, jnp.float32), -5.0, 5.0)
    return values.astype(jnp.bfloat16)


def draw_residual(key, part):
    keys = jax.random.split(jax.random.fold_in(key, 77), 4)
    column_pos = jnp.arange(DWIN, dtype=jnp.float32) / DWIN
    rising = 1.0 + (math.sqrt(3.0) - 1.0) * column_pos
    row_scale = jnp.exp(jax.random.uniform(keys[0], (ROWS, 1), jnp.float32, math.log(0.3), math.log(3.0)))
    column_scale = jnp.exp(jax.random.uniform(keys[1], (1, DWIN), jnp.float32, math.log(0.3), math.log(3.0))) * rising
    base = jnp.clip(jax.random.normal(keys[3], (ROWS, DWIN), jnp.float32), -5.0, 5.0)
    return (base * row_scale * column_scale).astype(jnp.bfloat16)


def with_ends(drawn, key, low, high):
    shape = drawn.shape
    place = [jax.random.randint(jax.random.fold_in(key, axis), (), 0, shape[axis]) for axis in range(len(shape))]
    drawn = drawn.at[tuple(place)].set(low)
    longest = shape.index(max(shape))
    place[longest] = (place[longest] + 1) % shape[longest]
    return drawn.at[tuple(place)].set(high)


def shard_levels(key, extent, cuts, smallest, top_value):
    gain = 1.0
    for position, shards_of in cuts:
        heights = jax.random.uniform(jax.random.fold_in(jax.random.fold_in(key, 6), position), (shards_of,), jnp.float32, smallest / len(cuts), top_value / len(cuts))
        gain = gain * jnp.repeat(jnp.exp(heights), extent[position] // shards_of).reshape((-1,) + (1,) * (len(extent) - 1 - position))
    return gain


def scatter_about(stream_key, extent, spread, limit, pieces=(), kind=jnp.bfloat16):
    gain = shard_levels(stream_key, extent, pieces, -0.22, 0.18) if pieces else 1.0
    result = jax.random.normal(stream_key, extent, jnp.float32) * spread * gain
    return jnp.minimum(jnp.maximum(result, -limit), limit).astype(kind)


def setup_inputs(seed: int = 0) -> dict:
    key_list = jax.random.split(jax.random.key(seed), 12)
    queries = draw_queries(jax.random.fold_in(key_list[11], 71), 0)
    draft_kv = draw_draft_kv(jax.random.fold_in(key_list[11], 71), 0)
    kv_pool = scatter_about(key_list[2], (POOL, 2, KVH, P_SIZE, HD), 1.0, 5.0, ((0, 32), (2, 8)))
    block_dest = draw_block_dest(jax.random.fold_in(key_list[11], 71), 0)
    block_table = draw_block_table(jax.random.fold_in(key_list[11], 71), 0)
    context_len = draw_context_len(jax.random.fold_in(key_list[11], 71), 0)
    draft_len = with_ends(jax.random.randint(key_list[6], (REQUESTS,), 2, W + 1), jax.random.fold_in(key_list[6], 1), 2, W).astype(jnp.int32)
    accept_mask = with_ends((jax.random.randint(key_list[7], (REQUESTS, W), 0, 8) < 7).astype(jnp.int32), jax.random.fold_in(key_list[7], 1), 0, 1)
    out_weight = scatter_about(key_list[8], (QH * HD, DWIN), HD ** -0.5, 0.5, ((0, 8),))
    residual = draw_residual(jax.random.fold_in(key_list[11], 71), 0)
    norm_gain = jnp.clip(1.0 + 0.18 * jax.random.normal(key_list[10], (DWIN,), jnp.float32), 0.1, 1.9)
    return dict(queries=queries, draft_kv=draft_kv, kv_pool=kv_pool, block_dest=block_dest, block_table=block_table, context_len=context_len, draft_len=draft_len, accept_mask=accept_mask, out_weight=out_weight, residual=residual, norm_gain=norm_gain)


masked_score = -1e+30
norm_epsilon = 1e-05

def move_anchor(block_dest):
    rank_count = N_DP
    destination = block_dest.reshape(rank_count, NB_DEV)
    columns = jnp.arange(rank_count, dtype=jnp.int32)
    onehot = (destination[:, :, None] == columns[None, None, :]).astype(jnp.int32)
    earlier = jnp.cumsum(onehot, axis=1, dtype=jnp.int32) - onehot
    order_in = lax.optimization_barrier(jnp.sum(earlier * onehot, axis=2, dtype=jnp.int32))
    source_rank = columns[:, None]
    target = jnp.where(destination >= 0, destination * (rank_count * SLOTS) + source_rank * SLOTS + order_in, rank_count * rank_count * SLOTS)
    anchor = jnp.full((rank_count * rank_count * SLOTS,), -1, jnp.int32)
    return anchor.at[target.reshape(-1)].set(jnp.arange(rank_count * NB_DEV, dtype=jnp.int32), mode='drop')

def reference(queries, draft_kv, kv_pool, block_dest, block_table, context_len, draft_len, accept_mask, out_weight, residual, norm_gain):
    group_size = QH // KVH
    scale_factor = 1.0 / math.sqrt(HD)
    anchor = move_anchor(block_dest)
    kept_count = lax.optimization_barrier(jnp.sum(jnp.cumprod(accept_mask, axis=1, dtype=jnp.int32), axis=1, dtype=jnp.int32))
    visible_limit = context_len - W + kept_count
    owner_rank = jnp.arange(REQUESTS, dtype=jnp.int32) // REQ
    positions = jnp.arange(MAXB, dtype=jnp.int32)[:, None] * P_SIZE + jnp.arange(P_SIZE, dtype=jnp.int32)[None, :]
    causal = jnp.arange(W, dtype=jnp.int32)[None, :] <= jnp.arange(W, dtype=jnp.int32)[:, None]
    highest = lax.Precision.HIGHEST

    def attend(request_item):
        query_heads, drafts, table_row, visible, owner = request_item
        slot_index = anchor[owner * (N_DP * SLOTS) + table_row]
        slot_found = (slot_index >= 0).astype(jnp.float32)
        blocks = kv_pool[jnp.maximum(slot_index, 0)].astype(jnp.float32) * slot_found[:, None, None, None, None]
        cached_keys = blocks[:, 0]
        cached_values = blocks[:, 1]
        grouped = query_heads.astype(jnp.float32).reshape(KVH, group_size, W, HD)
        cached = jnp.einsum('kgwd,bkpd->kgwbp', grouped, cached_keys, precision=highest) * scale_factor
        cached = jnp.where((positions < visible)[None, None, None], cached, masked_score)
        draft_keys = drafts[0].astype(jnp.float32)
        draft_values = drafts[1].astype(jnp.float32)
        draft_scores = jnp.einsum('kgwd,kjd->kgwj', grouped, draft_keys, precision=highest) * scale_factor
        draft_scores = jnp.where(causal[None, None], draft_scores, masked_score)
        row_max = jnp.maximum(lax.optimization_barrier(jnp.max(cached, axis=(3, 4))), lax.optimization_barrier(jnp.max(draft_scores, axis=3)))
        cached_exp = jnp.exp(cached - row_max[..., None, None])
        draft_exp = jnp.exp(draft_scores - row_max[..., None])
        denominator = lax.optimization_barrier(jnp.sum(cached_exp, axis=(3, 4))) + lax.optimization_barrier(jnp.sum(draft_exp, axis=3))
        cached_prob = lax.optimization_barrier((cached_exp / denominator[..., None, None]).astype(jnp.bfloat16)).astype(jnp.float32)
        draft_prob = lax.optimization_barrier((draft_exp / denominator[..., None]).astype(jnp.bfloat16)).astype(jnp.float32)
        attended = jnp.einsum('kgwbp,bkpd->kgwd', cached_prob, cached_values, precision=highest)
        attended = attended + jnp.einsum('kgwj,kjd->kgwd', draft_prob, draft_values, precision=highest)
        return attended.astype(jnp.bfloat16).reshape(QH, W, HD)
    attention = lax.map(attend, (queries, draft_kv, block_table, visible_limit, owner_rank))
    token_rows = attention.transpose(0, 2, 1, 3).reshape(ROWS, QH * HD)
    head_width = QH // N_MP * HD
    hidden = residual.astype(jnp.float32)
    for shard_index in range(N_MP):
        partial_value = jnp.dot(token_rows[:, shard_index * head_width:(shard_index + 1) * head_width], out_weight[shard_index * head_width:(shard_index + 1) * head_width], preferred_element_type=jnp.float32)
        hidden = hidden + lax.optimization_barrier(partial_value.astype(jnp.bfloat16)).astype(jnp.float32)
    mean_square = lax.optimization_barrier(jnp.mean(hidden * hidden, axis=1, keepdims=True))
    normed = hidden * lax.rsqrt(mean_square + norm_epsilon) * norm_gain[None, :]
    live_rows = (jnp.arange(W, dtype=jnp.int32)[None, :] < draft_len[:, None]).reshape(ROWS)
    return jnp.where(live_rows[:, None], normed, 0.0).astype(jnp.bfloat16)
```

```python
import functools
import math

import jax
import jax.numpy as jnp
from jax import lax
from jax.experimental import pallas as pl
from jax.experimental.pallas import tpu as pltpu
from jax.sharding import PartitionSpec as P

masked_score = -1e30
norm_epsilon = 1e-05
load_pieces = 8


def from_everyone(array, axis):
    length = lax.axis_size(axis)
    return lax.all_to_all(
        jnp.broadcast_to(array[None], (length, *array.shape)), axis, 0, 0, tiled=True
    )


def over_copies(array, axis):
    everything = from_everyone(array, axis)
    return jnp.sum(everything, axis=0)


def pack_kernel(rank_count, capacity, dest_ref, pool_ref, out_ref, staged, used, load_sem, store_sem):
    blocks = pool_ref.shape[0]
    piece = blocks // load_pieces

    def load(p):
        rows = pl.ds(p * piece, piece)
        return pltpu.make_async_copy(pool_ref.at[rows], staged.at[rows], load_sem.at[p])

    for p in range(load_pieces):
        load(p).start()

    def clear(d, carry):
        used[d] = 0
        return carry

    lax.fori_loop(0, rank_count, clear, 0)

    def store(b, slot):
        return pltpu.make_async_copy(staged.at[b], out_ref.at[slot], store_sem)

    def place(b, sent):
        d = dest_ref[b]
        live = d >= 0

        @pl.when(live)
        def _():
            k = used[d]
            used[d] = k + 1
            store(b, d * capacity + k).start()

        return sent + live.astype(jnp.int32)

    sent = jnp.int32(0)
    for p in range(load_pieces):
        load(p).wait()
        sent = lax.fori_loop(p * piece, (p + 1) * piece, place, sent, unroll=4)

    def drain(i, carry):
        store(0, 0).wait()
        return carry

    lax.fori_loop(0, sent, drain, 0)


def pack_blocks(block_dest, pool, rank_count, capacity):
    return pl.pallas_call(
        functools.partial(pack_kernel, rank_count, capacity),
        out_shape=jax.ShapeDtypeStruct((rank_count * capacity,) + pool.shape[1:], pool.dtype),
        in_specs=[
            pl.BlockSpec(memory_space=pltpu.SMEM),
            pl.BlockSpec(memory_space=pl.ANY),
        ],
        out_specs=pl.BlockSpec(memory_space=pl.ANY),
        scratch_shapes=[
            pltpu.VMEM(pool.shape, pool.dtype),
            pltpu.SMEM((rank_count,), jnp.int32),
            pltpu.SemaphoreType.DMA((load_pieces,)),
            pltpu.SemaphoreType.DMA,
        ],
        cost_estimate=pl.CostEstimate(flops=0, bytes_accessed=1 << 23, transcendentals=0),
        name="pack_blocks",
    )(block_dest, pool)


def attend_kernel(per_step, table_ref, visible_ref, queries_ref, draft_ref, arrived_ref, out_ref, cache, load_sem):
    slots = arrived_ref.shape[0]
    step = pl.program_id(0)
    width = table_ref.shape[0] // visible_ref.shape[0]
    block_len = arrived_ref.shape[1] // 2
    rows, head_dim = queries_ref.shape[1:]
    window = out_ref.shape[0] // per_step
    log_scale = math.log2(math.e) / math.sqrt(head_dim)

    @pl.when(step == 0)
    def _():
        piece = slots // load_pieces
        copies = [
            pltpu.make_async_copy(
                arrived_ref.at[pl.ds(p * piece, piece)],
                cache.at[pl.ds(p * piece, piece)],
                load_sem.at[p],
            )
            for p in range(load_pieces)
        ]
        for copy in copies:
            copy.start()
        cache[slots] = jnp.zeros_like(cache[slots])
        for copy in copies:
            copy.wait()

    positions = lax.broadcasted_iota(jnp.int32, (rows, width * block_len), 1)
    query_place = lax.broadcasted_iota(jnp.int32, (rows, window), 0) % window
    causal = lax.broadcasted_iota(jnp.int32, (rows, window), 1) <= query_place
    over_last = (((1,), (1,)), ((), ()))
    for n in range(per_step):
        request = step * per_step + n
        visible = visible_ref[request]
        places = [
            jnp.where(e * block_len < visible, table_ref[request * width + e], slots)
            for e in range(width)
        ]
        keys = jnp.concatenate([cache[s, :block_len, :] for s in places], axis=0)
        values = jnp.concatenate([cache[s, block_len:, :] for s in places], axis=0)
        query = queries_ref[n]
        cached = lax.dot_general(query, keys, over_last, preferred_element_type=jnp.float32)
        cached = jnp.where(positions < visible, cached, masked_score)
        drafts = lax.dot_general(
            query, draft_ref[n, :window, :], over_last, preferred_element_type=jnp.float32
        )
        drafts = jnp.where(causal, drafts, masked_score)
        row_max = jnp.maximum(
            jnp.max(cached, axis=1, keepdims=True), jnp.max(drafts, axis=1, keepdims=True)
        )
        cached = jnp.exp2((cached - row_max) * log_scale)
        drafts = jnp.exp2((drafts - row_max) * log_scale)
        denominator = jnp.sum(cached, axis=1, keepdims=True) + jnp.sum(drafts, axis=1, keepdims=True)
        attended = jnp.dot(cached.astype(jnp.bfloat16), values, preferred_element_type=jnp.float32)
        attended = attended + jnp.dot(
            drafts.astype(jnp.bfloat16), draft_ref[n, window:, :], preferred_element_type=jnp.float32
        )
        attended = (attended / denominator).astype(jnp.bfloat16)
        for h in range(rows // window):
            out_ref[n * window : (n + 1) * window, h * head_dim : (h + 1) * head_dim] = attended[
                h * window : (h + 1) * window
            ]


def attend(table, visible, queries, drafts, arrived, window, per_step=2):
    requests, rows, head_dim = queries.shape
    slots = arrived.shape[0]
    return pl.pallas_call(
        functools.partial(attend_kernel, per_step),
        out_shape=jax.ShapeDtypeStruct((requests * window, rows // window * head_dim), jnp.bfloat16),
        grid_spec=pltpu.PrefetchScalarGridSpec(
            num_scalar_prefetch=2,
            grid=(requests // per_step,),
            in_specs=[
                pl.BlockSpec((per_step, rows, head_dim), lambda i, *_: (i, 0, 0)),
                pl.BlockSpec((per_step,) + drafts.shape[1:], lambda i, *_: (i, 0, 0)),
                pl.BlockSpec(memory_space=pl.ANY),
            ],
            out_specs=pl.BlockSpec(
                (per_step * window, rows // window * head_dim), lambda i, *_: (i, 0)
            ),
            scratch_shapes=[
                pltpu.VMEM((slots + 1,) + arrived.shape[1:], arrived.dtype),
                pltpu.SemaphoreType.DMA((load_pieces,)),
            ],
        ),
        cost_estimate=pl.CostEstimate(flops=1 << 30, bytes_accessed=10 << 20, transcendentals=1 << 21),
        name="attend",
    )(table, visible, queries, drafts, arrived)


def on_device(
    queries,
    draft_kv,
    kv_pool,
    block_dest,
    block_table,
    context_len,
    draft_len,
    accept_mask,
    out_weight,
    residual,
    norm_gain,
):
    rank_count = lax.axis_size("dp")
    pool_count = kv_pool.shape[0]
    capacity = 2 * pool_count // rank_count
    requests, heads_local, window, head_dim = queries.shape
    block_len = kv_pool.shape[3]
    pool = kv_pool.reshape(pool_count, 2 * block_len, head_dim)
    outgoing = pack_blocks(block_dest, pool, rank_count, capacity)
    arrived = lax.all_to_all(outgoing, "dp", split_axis=0, concat_axis=0, tiled=True)
    kept_count = jnp.sum(jnp.cumprod(accept_mask, axis=1, dtype=jnp.int32), axis=1, dtype=jnp.int32)
    visible = context_len - window + kept_count
    token_rows = attend(
        block_table.reshape(-1),
        visible,
        queries.reshape(requests, heads_local * window, head_dim),
        draft_kv.reshape(requests, 2 * window, head_dim),
        arrived,
        window,
    )
    partial_value = jnp.dot(token_rows, out_weight, preferred_element_type=jnp.float32)
    column_count = norm_gain.shape[0]
    column_start = lax.axis_index("mp") * column_count
    live_rows = (jnp.arange(window, dtype=jnp.int32)[None, :] < draft_len[:, None]).reshape(
        requests * window
    )
    share = lax.psum_scatter(
        partial_value.astype(jnp.bfloat16), "mp", scatter_dimension=1, tiled=True
    ).astype(jnp.float32)
    local_residual = lax.dynamic_slice_in_dim(residual, column_start, column_count, 1)
    local_hidden = local_residual.astype(jnp.float32) + share
    squares = over_copies(jnp.sum(local_hidden * local_hidden, axis=1), "mp")
    mean_square = (squares / (column_count * lax.axis_size("mp")))[:, None]
    normed = local_hidden * lax.rsqrt(mean_square + norm_epsilon) * norm_gain[None, :]
    return jnp.where(live_rows[:, None], normed, 0.0).astype(jnp.bfloat16)


def solution(mesh):
    return jax.shard_map(
        on_device,
        mesh=mesh,
        in_specs=(
            P("dp", "mp", None, None),
            P("dp", None, "mp", None, None),
            P("dp", None, "mp", None, None),
            P("dp"),
            P("dp", None),
            P("dp"),
            P("dp"),
            P("dp", None),
            P("mp", None),
            P("dp", None),
            P("mp"),
        ),
        out_specs=P("dp", "mp"),
        check_vma=False,
    )
```

```python
import functools
import math

import jax
import jax.numpy as jnp
from jax import lax
from jax.experimental import pallas as pl
from jax.experimental.pallas import tpu as pltpu
from jax.sharding import PartitionSpec as P

masked_score = -1e30
norm_epsilon = 1e-05
load_pieces = 8


def from_everyone(array, axis):
    length = lax.axis_size(axis)
    return lax.all_to_all(
        jnp.broadcast_to(array[None], (length, *array.shape)), axis, 0, 0, tiled=True
    )


def over_copies(array, axis):
    everything = from_everyone(array, axis)
    return jnp.sum(everything, axis=0)


def pack_kernel(rank_count, capacity, dest_ref, pool_ref, out_ref, staged, used, load_sem, store_sem):
    blocks = pool_ref.shape[0]
    piece = blocks // load_pieces

    def load(p):
        rows = pl.ds(p * piece, piece)
        return pltpu.make_async_copy(pool_ref.at[rows], staged.at[rows], load_sem.at[p])

    for p in range(load_pieces):
        load(p).start()

    def clear(d, carry):
        used[d] = 0
        return carry

    lax.fori_loop(0, rank_count, clear, 0)

    def store(b, slot):
        return pltpu.make_async_copy(staged.at[b], out_ref.at[slot], store_sem)

    def place(b, sent):
        d = dest_ref[b]
        live = d >= 0

        @pl.when(live)
        def _():
            k = used[d]
            used[d] = k + 1
            store(b, d * capacity + k).start()

        return sent + live.astype(jnp.int32)

    sent = jnp.int32(0)
    for p in range(load_pieces):
        load(p).wait()
        sent = lax.fori_loop(p * piece, (p + 1) * piece, place, sent, unroll=4)

    def drain(i, carry):
        store(0, 0).wait()
        return carry

    lax.fori_loop(0, sent, drain, 0)


def pack_blocks(block_dest, pool, rank_count, capacity):
    return pl.pallas_call(
        functools.partial(pack_kernel, rank_count, capacity),
        out_shape=jax.ShapeDtypeStruct((rank_count * capacity,) + pool.shape[1:], pool.dtype),
        in_specs=[
            pl.BlockSpec(memory_space=pltpu.SMEM),
            pl.BlockSpec(memory_space=pl.ANY),
        ],
        out_specs=pl.BlockSpec(memory_space=pl.ANY),
        scratch_shapes=[
            pltpu.VMEM(pool.shape, pool.dtype),
            pltpu.SMEM((rank_count,), jnp.int32),
            pltpu.SemaphoreType.DMA((load_pieces,)),
            pltpu.SemaphoreType.DMA,
        ],
        cost_estimate=pl.CostEstimate(flops=0, bytes_accessed=1 << 23, transcendentals=0),
        name="pack_blocks",
    )(block_dest, pool)


def attend_kernel(per_step, table_ref, visible_ref, queries_ref, draft_ref, arrived_ref, out_ref, cache, load_sem):
    slots = arrived_ref.shape[0]
    step = pl.program_id(0)
    width = table_ref.shape[0] // visible_ref.shape[0]
    block_len = arrived_ref.shape[1] // 2
    rows, head_dim = queries_ref.shape[1:]
    window = out_ref.shape[0] // per_step
    log_scale = math.log2(math.e) / math.sqrt(head_dim)

    @pl.when(step == 0)
    def _():
        piece = slots // load_pieces
        copies = [
            pltpu.make_async_copy(
                arrived_ref.at[pl.ds(p * piece, piece)],
                cache.at[pl.ds(p * piece, piece)],
                load_sem.at[p],
            )
            for p in range(load_pieces)
        ]
        for copy in copies:
            copy.start()
        cache[slots] = jnp.zeros_like(cache[slots])
        for copy in copies:
            copy.wait()

    positions = lax.broadcasted_iota(jnp.int32, (rows, width * block_len), 1)
    query_place = lax.broadcasted_iota(jnp.int32, (rows, window), 0) % window
    causal = lax.broadcasted_iota(jnp.int32, (rows, window), 1) <= query_place
    over_last = (((1,), (1,)), ((), ()))
    for n in range(per_step):
        request = step * per_step + n
        visible = visible_ref[request]
        places = [
            jnp.where(e * block_len < visible, table_ref[request * width + e], slots)
            for e in range(width)
        ]
        keys = jnp.concatenate([cache[s, :block_len, :] for s in places], axis=0)
        values = jnp.concatenate([cache[s, block_len:, :] for s in places], axis=0)
        query = queries_ref[n]
        cached = lax.dot_general(query, keys, over_last, preferred_element_type=jnp.float32)
        cached = jnp.where(positions < visible, cached, masked_score)
        drafts = lax.dot_general(
            query, draft_ref[n, :window, :], over_last, preferred_element_type=jnp.float32
        )
        drafts = jnp.where(causal, drafts, masked_score)
        row_max = jnp.maximum(
            jnp.max(cached, axis=1, keepdims=True), jnp.max(drafts, axis=1, keepdims=True)
        )
        cached = jnp.exp2((cached - row_max) * log_scale)
        drafts = jnp.exp2((drafts - row_max) * log_scale)
        denominator = jnp.sum(cached, axis=1, keepdims=True) + jnp.sum(drafts, axis=1, keepdims=True)
        attended = jnp.dot(cached.astype(jnp.bfloat16), values, preferred_element_type=jnp.float32)
        attended = attended + jnp.dot(
            drafts.astype(jnp.bfloat16), draft_ref[n, window:, :], preferred_element_type=jnp.float32
        )
        attended = (attended / denominator).astype(jnp.bfloat16)
        for h in range(rows // window):
            out_ref[n * window : (n + 1) * window, h * head_dim : (h + 1) * head_dim] = attended[
                h * window : (h + 1) * window
            ]


def attend(table, visible, queries, drafts, arrived, window, per_step=2):
    requests, rows, head_dim = queries.shape
    slots = arrived.shape[0]
    return pl.pallas_call(
        functools.partial(attend_kernel, per_step),
        out_shape=jax.ShapeDtypeStruct((requests * window, rows // window * head_dim), jnp.bfloat16),
        grid_spec=pltpu.PrefetchScalarGridSpec(
            num_scalar_prefetch=2,
            grid=(requests // per_step,),
            in_specs=[
                pl.BlockSpec((per_step, rows, head_dim), lambda i, *_: (i, 0, 0)),
                pl.BlockSpec((per_step,) + drafts.shape[1:], lambda i, *_: (i, 0, 0)),
                pl.BlockSpec(memory_space=pl.ANY),
            ],
            out_specs=pl.BlockSpec(
                (per_step * window, rows // window * head_dim), lambda i, *_: (i, 0)
            ),
            scratch_shapes=[
                pltpu.VMEM((slots + 1,) + arrived.shape[1:], arrived.dtype),
                pltpu.SemaphoreType.DMA((load_pieces,)),
            ],
        ),
        cost_estimate=pl.CostEstimate(flops=1 << 30, bytes_accessed=10 << 20, transcendentals=1 << 21),
        name="attend",
    )(table, visible, queries, drafts, arrived)


def project(token_rows, out_weight, column_count):
    size = lax.axis_size("mp")
    chips = size // 2
    place = lax.axis_index("mp")
    core = place % 2
    swap = [(i, i ^ 1) for i in range(size)]
    right = [(i, (i + 2) % size) for i in range(size)]
    left = [(i, (i - 2) % size) for i in range(size)]

    def columns(k, c):
        chip = (place // 2 + k) % chips
        return lax.dynamic_slice_in_dim(out_weight, (chip * 2 + c) * column_count, column_count, 1)

    own_weight = [columns(k, core) for k in range(chips)]
    given = jnp.concatenate([columns(k, 1 - core) for k in range(chips)], axis=0)
    their_weight = jnp.split(lax.ppermute(given, "mp", swap), chips, axis=0)
    theirs = lax.ppermute(token_rows, "mp", swap)

    def partial(k):
        own = jnp.dot(token_rows, own_weight[k], preferred_element_type=jnp.float32)
        return own + jnp.dot(theirs, their_weight[k], preferred_element_type=jnp.float32)

    half = column_count // 2
    far = partial(2).astype(jnp.bfloat16)
    from_left = lax.ppermute(far[:, :half], "mp", right)
    from_right = lax.ppermute(far[:, half:], "mp", left)
    ahead = partial(1)
    behind = partial(3)
    home = partial(0)
    ahead = jnp.concatenate([ahead[:, :half] + from_left.astype(jnp.float32), ahead[:, half:]], axis=1)
    behind = jnp.concatenate([behind[:, :half], behind[:, half:] + from_right.astype(jnp.float32)], axis=1)
    from_left = lax.ppermute(ahead.astype(jnp.bfloat16), "mp", right)
    from_right = lax.ppermute(behind.astype(jnp.bfloat16), "mp", left)
    return home + from_left.astype(jnp.float32) + from_right.astype(jnp.float32)


def on_device(
    queries,
    draft_kv,
    kv_pool,
    block_dest,
    block_table,
    context_len,
    draft_len,
    accept_mask,
    out_weight,
    residual,
    norm_gain,
):
    rank_count = lax.axis_size("dp")
    pool_count = kv_pool.shape[0]
    capacity = 2 * pool_count // rank_count
    requests, heads_local, window, head_dim = queries.shape
    block_len = kv_pool.shape[3]
    pool = kv_pool.reshape(pool_count, 2 * block_len, head_dim)
    outgoing = pack_blocks(block_dest, pool, rank_count, capacity)
    arrived = lax.all_to_all(outgoing, "dp", split_axis=0, concat_axis=0, tiled=True)
    kept_count = jnp.sum(jnp.cumprod(accept_mask, axis=1, dtype=jnp.int32), axis=1, dtype=jnp.int32)
    visible = context_len - window + kept_count
    token_rows = attend(
        block_table.reshape(-1),
        visible,
        queries.reshape(requests, heads_local * window, head_dim),
        draft_kv.reshape(requests, 2 * window, head_dim),
        arrived,
        window,
    )
    column_count = norm_gain.shape[0]
    place = lax.axis_index("mp")
    live_rows = (jnp.arange(window, dtype=jnp.int32)[None, :] < draft_len[:, None]).reshape(
        requests * window
    )
    share = project(token_rows, out_weight, column_count)
    local_residual = lax.dynamic_slice_in_dim(residual, place * column_count, column_count, 1)
    local_hidden = local_residual.astype(jnp.float32) + share
    squares = over_copies(jnp.sum(local_hidden * local_hidden, axis=1), "mp")
    mean_square = (squares / (column_count * lax.axis_size("mp")))[:, None]
    normed = local_hidden * lax.rsqrt(mean_square + norm_epsilon) * norm_gain[None, :]
    return jnp.where(live_rows[:, None], normed, 0.0).astype(jnp.bfloat16)


def solution(mesh):
    return jax.shard_map(
        on_device,
        mesh=mesh,
        in_specs=(
            P("dp", "mp", None, None),
            P("dp", None, "mp", None, None),
            P("dp", None, "mp", None, None),
            P("dp"),
            P("dp", None),
            P("dp"),
            P("dp"),
            P("dp", None),
            P("mp", None),
            P("dp", None),
            P("mp"),
        ),
        out_specs=P("dp", "mp"),
        check_vma=False,
    )
```

```python
import functools
import math

import jax
import jax.numpy as jnp
from jax import lax
from jax.experimental import pallas as pl
from jax.experimental.pallas import tpu as pltpu
from jax.sharding import PartitionSpec as P


masked_score = -1e30
norm_epsilon = 1e-05
load_pieces = 2
ring_len = 8
room = (168, 168, 124, 52)


def over(array, power):
    return lax.shift_right_arithmetic(array, jnp.int32(power.bit_length() - 1))


def rest(array, power):
    return jnp.bitwise_and(array, power - 1)


def from_everyone(array, axis):
    length = lax.axis_size(axis)
    return lax.all_to_all(
        jnp.broadcast_to(array[None], (length, *array.shape)), axis, 0, 0, tiled=True
    )


def over_copies(array, axis):
    everything = from_everyone(array, axis)
    return jnp.sum(everything, axis=0)


def pack_kernel(halved, kinds, dest_ref, start_ref, pool_ref, *refs):
    outs, (staged, used, sem, out_sem) = refs[:-4], refs[-4:]
    blocks = pool_ref.shape[0]
    slots = staged.shape[0] - blocks

    def clear(d, carry):
        used[d] = 0
        return carry

    lax.fori_loop(0, kinds + 1, clear, 0)

    def place(b, carry):
        d = dest_ref[b]
        k = used[d]
        used[d] = k + 1
        slot = start_ref[2 * d + (k & 1)] + jnp.where(halved(d), k >> 1, k)
        slot = jnp.where(d < kinds, jnp.minimum(slot, slots - 1), slots + b)
        pltpu.make_async_copy(pool_ref.at[b], staged.at[slot], sem).start()
        return carry

    lax.fori_loop(0, blocks, place, 0, unroll=4 if len(outs) > 1 else 1)
    pltpu.make_async_copy(pool_ref, staged.at[pl.ds(0, blocks)], sem).wait()
    copies, at = [], 0
    for n, out in enumerate(outs):
        rows = pl.ds(at, out.shape[0])
        copies.append(pltpu.make_async_copy(staged.at[rows], out, out_sem.at[n]))
        at += out.shape[0]
    for copy in copies:
        copy.start()
    for copy in copies:
        copy.wait()


def pack_blocks(dest, start, pool, sizes, halved):
    kinds = start.shape[0] // 2 - 1
    return pl.pallas_call(
        functools.partial(pack_kernel, halved, kinds),
        out_shape=[jax.ShapeDtypeStruct((n,) + pool.shape[1:], pool.dtype) for n in sizes],
        in_specs=[
            pl.BlockSpec(memory_space=pltpu.SMEM),
            pl.BlockSpec(memory_space=pltpu.SMEM),
            pl.BlockSpec(memory_space=pl.ANY),
        ],
        out_specs=[pl.BlockSpec(memory_space=pl.ANY)] * len(sizes),
        scratch_shapes=[
            pltpu.VMEM((sum(sizes) + pool.shape[0],) + pool.shape[1:], pool.dtype),
            pltpu.SMEM((kinds + 1,), jnp.int32),
            pltpu.SemaphoreType.DMA,
            pltpu.SemaphoreType.DMA((len(sizes),)),
        ],
        cost_estimate=pl.CostEstimate(flops=1 << 28, bytes_accessed=1 << 23, transcendentals=0),
        name="pack_blocks",
    )(dest, start, pool)


def pick_kernel(plans, offset_ref, *refs):
    sources, outs, sem = refs[: -len(plans) - 1], refs[-len(plans) - 1 : -1], refs[-1]
    copies = []
    for plan, out in zip(plans, outs):
        at = 0
        for source, (kind, number), length in plan:
            start = offset_ref[number] if kind == "offset" else number
            copies.append(
                pltpu.make_async_copy(
                    sources[source].at[pl.ds(start, length)],
                    out.at[pl.ds(at, length)],
                    sem.at[len(copies)],
                )
            )
            at += length
    for copy in copies:
        copy.start()
    for copy in copies:
        copy.wait()


def pick(offsets, sources, plans):
    shape = sources[0].shape[1:]
    sizes = [sum(length for _, _, length in plan) for plan in plans]
    return pl.pallas_call(
        functools.partial(pick_kernel, plans),
        out_shape=[jax.ShapeDtypeStruct((n,) + shape, sources[0].dtype) for n in sizes],
        in_specs=[pl.BlockSpec(memory_space=pltpu.SMEM)]
        + [pl.BlockSpec(memory_space=pl.ANY)] * len(sources),
        out_specs=[pl.BlockSpec(memory_space=pltpu.VMEM)] * len(plans),
        scratch_shapes=[pltpu.SemaphoreType.DMA((sum(len(plan) for plan in plans),))],
        cost_estimate=pl.CostEstimate(flops=1 << 20, bytes_accessed=4 << 20, transcendentals=0),
        name="pick",
    )(offsets, *sources)


def attend_kernel(per_step, plan, table_ref, visible_ref, offset_ref, queries_ref, draft_ref, *refs):
    sources, (out_ref, cache, load_sem) = refs[:-3], refs[-3:]
    slots = cache.shape[0] - 1
    step = pl.program_id(0)
    width = table_ref.shape[0] // visible_ref.shape[0]
    block_len = cache.shape[1] // 2
    rows, head_dim = queries_ref.shape[1:]
    window = out_ref.shape[0] // per_step
    log_scale = math.log2(math.e) / math.sqrt(head_dim)

    @pl.when(step == 0)
    def _():
        copies, at = [], 0
        for source, (kind, number), length in plan:
            start = offset_ref[number] if kind == "offset" else number
            copies.append(
                pltpu.make_async_copy(
                    sources[source].at[pl.ds(start, length)],
                    cache.at[pl.ds(at, length)],
                    load_sem.at[len(copies)],
                )
            )
            at += length
        for copy in copies:
            copy.start()
        cache[slots] = jnp.zeros_like(cache[slots])
        for copy in copies:
            copy.wait()

    positions = lax.broadcasted_iota(jnp.int32, (rows, width * block_len), 1)
    query_place = rest(lax.broadcasted_iota(jnp.int32, (rows, window), 0), window)
    causal = lax.broadcasted_iota(jnp.int32, (rows, window), 1) <= query_place
    over_last = (((1,), (1,)), ((), ()))
    for n in range(per_step):
        request = step * per_step + n
        visible = visible_ref[request]
        places = [
            jnp.where(e * block_len < visible, table_ref[request * width + e], slots)
            for e in range(width)
        ]
        keys = jnp.concatenate([cache[s, :block_len, :] for s in places], axis=0)
        values = jnp.concatenate([cache[s, block_len:, :] for s in places], axis=0)
        query = queries_ref[n]
        cached = lax.dot_general(query, keys, over_last, preferred_element_type=jnp.float32)
        cached = jnp.where(positions < visible, cached, masked_score)
        drafts = lax.dot_general(
            query, draft_ref[n, :window, :], over_last, preferred_element_type=jnp.float32
        )
        drafts = jnp.where(causal, drafts, masked_score)
        row_max = jnp.maximum(
            jnp.max(cached, axis=1, keepdims=True), jnp.max(drafts, axis=1, keepdims=True)
        )
        cached = jnp.exp2((cached - row_max) * log_scale)
        drafts = jnp.exp2((drafts - row_max) * log_scale)
        denominator = jnp.sum(cached, axis=1, keepdims=True) + jnp.sum(drafts, axis=1, keepdims=True)
        attended = jnp.dot(cached.astype(jnp.bfloat16), values, preferred_element_type=jnp.float32)
        attended = attended + jnp.dot(
            drafts.astype(jnp.bfloat16), draft_ref[n, window:, :], preferred_element_type=jnp.float32
        )
        attended = (attended / denominator).astype(jnp.bfloat16)
        for h in range(rows // window):
            out_ref[n * window : (n + 1) * window, h * head_dim : (h + 1) * head_dim] = attended[
                h * window : (h + 1) * window
            ]


def attend(table, visible, offsets, queries, drafts, sources, plan, window, per_step=2):
    requests, rows, head_dim = queries.shape
    slots = sum(length for _, _, length in plan)
    return pl.pallas_call(
        functools.partial(attend_kernel, per_step, plan),
        out_shape=jax.ShapeDtypeStruct((requests * window, rows // window * head_dim), jnp.bfloat16),
        grid_spec=pltpu.PrefetchScalarGridSpec(
            num_scalar_prefetch=3,
            grid=(requests // per_step,),
            in_specs=[
                pl.BlockSpec((per_step, rows, head_dim), lambda i, *_: (i, 0, 0)),
                pl.BlockSpec((per_step,) + drafts.shape[1:], lambda i, *_: (i, 0, 0)),
            ]
            + [pl.BlockSpec(memory_space=pl.ANY)] * len(sources),
            out_specs=pl.BlockSpec(
                (per_step * window, rows // window * head_dim), lambda i, *_: (i, 0)
            ),
            scratch_shapes=[
                pltpu.VMEM((slots + 1,) + sources[0].shape[1:], sources[0].dtype),
                pltpu.SemaphoreType.DMA((len(plan),)),
            ],
        ),
        cost_estimate=pl.CostEstimate(flops=1 << 30, bytes_accessed=10 << 20, transcendentals=1 << 21),
        name="attend",
    )(table, visible, offsets, queries, drafts, *sources)


def ring_starts(counts):
    middle = counts[..., 4]
    up = jnp.stack([over(middle + 1, 2), counts[..., 3], counts[..., 2]], axis=-2)
    down = jnp.stack([over(middle, 2), counts[..., 5], counts[..., 6]], axis=-2)
    both = jnp.stack([up, down], axis=-3)
    flat = both.reshape(both.shape[:-2] + (12,))
    before = (jnp.arange(12)[:, None] < jnp.arange(12)[None, :]).astype(jnp.int32)
    starts = jnp.sum(flat[..., :, None] * before, axis=-2).reshape(both.shape)
    group = both.sum(axis=-1)
    upto = (jnp.arange(3)[:, None] <= jnp.arange(3)[None, :]).astype(jnp.int32)
    travelling = jnp.sum(group[..., :, None] * upto, axis=-2)
    return starts, travelling


def by_distance(near, up, down, axis):
    part = lambda array, g: lax.slice_in_dim(array, g, g + 1, axis=axis)
    tables = []
    for middle in (up, down):
        parts = [near[0], near[1], part(up, 2), part(up, 1), part(middle, 0), part(down, 1), part(down, 2), near[2]]
        tables.append(jnp.concatenate(parts, axis=axis))
    return tables


def neighbours(ring_len, y_len):
    size = y_len * ring_len
    return (
        [(i, i // ring_len * ring_len + (i + 1) % ring_len) for i in range(size)],
        [(i, i // ring_len * ring_len + (i - 1) % ring_len) for i in range(size)],
        [(i, (i + ring_len) % size) for i in range(size)],
        [(i, (i - ring_len) % size) for i in range(size)],
    )


def first_moves(outputs, along, full):
    own, for_forth, for_back, rising, falling = outputs
    up, down, forth, back = along
    for _ in range(1, 3):
        rising = lax.ppermute(rising, "dp", up)
        falling = lax.ppermute(falling, "dp", down)
    forth_0 = lax.ppermute(for_forth, "dp", forth)
    back_0 = lax.ppermute(for_back, "dp", back)
    forth_00 = lax.ppermute(lax.slice_in_dim(forth_0, 3 * full, 5 * full), "dp", forth)
    back_00 = lax.ppermute(lax.slice_in_dim(back_0, 3 * full, 4 * full), "dp", back)
    return own, forth_0, back_0, forth_00, back_00, rising, falling


def along_rings(carried, offsets, along, capacity, room):
    own, forth_0, back_0, forth_00, back_00, rising, falling = carried
    up, down, forth, back = along
    full, half = capacity, capacity // 2
    arrays = [own, forth_0, back_0, forth_00, back_00]
    home = [(0, ("at", 0), full), (1, ("at", 0), full), (3, ("at", 0), full), (2, ("at", 0), full)]
    for_up = [(0, ("at", full), full), (1, ("at", full), full), (3, ("at", full), full), (2, ("at", full), full)]
    for_down = [(0, ("at", 2 * full), full), (1, ("at", 2 * full), full), (4, ("at", 0), full), (2, ("at", 2 * full), full)]
    found = {}

    def keep(array):
        arrays.append(array)
        return len(arrays) - 1

    passing_forth = passing_back = None
    for t in range(2, 5):
        u, d = keep(rising), keep(falling)
        if t < 4:
            rising = lax.ppermute(lax.slice_in_dim(rising, 0, room[t]), "dp", up)
            falling = lax.ppermute(lax.slice_in_dim(falling, 0, room[t]), "dp", down)
        length = full if t < 4 else half

        def piece(direction, r):
            number = ((t - 2) * 2 + direction) * 4 + r
            return ((u, d)[direction], ("offset", number), length)

        found[0, t, 0], found[1, t, 0] = piece(0, 0), piece(1, 0)
        forward = [piece(0, 1), piece(1, 1), piece(0, 2)]
        backward = [piece(0, 3), piece(1, 3), piece(1, 2)]
        for plan, passing in ((forward, passing_forth), (backward, passing_back)):
            if passing is not None:
                plan.append((passing[0], ("at", passing[1]), passing[2]))
        needed = sorted({p[0] for p in forward + backward})
        renamed = [
            [(needed.index(source), start, n) for source, start, n in plan]
            for plan in (forward, backward)
        ]
        send_forth, send_back = pick(offsets, [arrays[i] for i in needed], renamed)
        f = keep(lax.ppermute(send_forth, "dp", forth))
        b = keep(lax.ppermute(send_back, "dp", back))
        found[0, t, 1], found[1, t, 1] = (f, ("at", 0), length), (f, ("at", length), length)
        found[0, t, 3], found[1, t, 3] = (b, ("at", 0), length), (b, ("at", length), length)
        if t > 2:
            found[0, t - 1, 2] = (f, ("at", 3 * length), full)
            found[1, t - 1, 2] = (b, ("at", 3 * length), full)
        passing_forth, passing_back = (f, 2 * length, length), (b, 2 * length, length)
    near_up, near_down = pick(offsets, arrays[:5], [for_up, for_down])
    near_up = keep(lax.ppermute(near_up, "dp", up))
    near_down = keep(lax.ppermute(near_down, "dp", down))
    last_forth = lax.slice_in_dim(arrays[passing_forth[0]], 2 * half, 3 * half)
    last_back = lax.slice_in_dim(arrays[passing_back[0]], 2 * half, 3 * half)
    found[0, 4, 2] = (keep(lax.ppermute(last_forth, "dp", forth)), ("at", 0), half)
    found[1, 4, 2] = (keep(lax.ppermute(last_back, "dp", back)), ("at", 0), half)
    plan = home + [(near_up, ("at", 0), 4 * full), (near_down, ("at", 0), 4 * full)]
    plan += [found[direction, t, r] for t in range(2, 5) for direction in range(2) for r in range(4)]
    return arrays, plan


def project(token_rows, out_weight, column_count):
    size = lax.axis_size("mp")
    chips = size // 2
    place = lax.axis_index("mp")
    core = rest(place, 2)
    swap = [(i, i ^ 1) for i in range(size)]
    right = [(i, (i + 2) % size) for i in range(size)]
    left = [(i, (i - 2) % size) for i in range(size)]

    def columns(k, c):
        chip = rest(over(place, 2) + k, chips)
        return lax.dynamic_slice_in_dim(out_weight, (chip * 2 + c) * column_count, column_count, 1)

    own_weight = [columns(k, core) for k in range(chips)]
    given = jnp.concatenate([columns(k, 1 - core) for k in range(chips)], axis=0)
    their_weight = jnp.split(lax.ppermute(given, "mp", swap), chips, axis=0)
    theirs = lax.ppermute(token_rows, "mp", swap)

    def own_part(k):
        own = jnp.dot(token_rows, own_weight[k], preferred_element_type=jnp.float32)
        return lax.optimization_barrier(own)

    own_far = own_part(2)
    own_ahead = own_part(1)

    def with_theirs(own, k):
        return own + jnp.dot(theirs, their_weight[k], preferred_element_type=jnp.float32)

    half = column_count // 2
    far = with_theirs(own_far, 2).astype(jnp.bfloat16)
    from_left = lax.ppermute(far[:, :half], "mp", right)
    from_right = lax.ppermute(far[:, half:], "mp", left)
    ahead = with_theirs(own_ahead, 1)
    behind = with_theirs(own_part(3), 3)
    home = with_theirs(own_part(0), 0)
    ahead = jnp.concatenate([ahead[:, :half] + from_left.astype(jnp.float32), ahead[:, half:]], axis=1)
    behind = jnp.concatenate([behind[:, :half], behind[:, half:] + from_right.astype(jnp.float32)], axis=1)
    from_left = lax.ppermute(ahead.astype(jnp.bfloat16), "mp", right)
    from_right = lax.ppermute(behind.astype(jnp.bfloat16), "mp", left)
    return home + from_left.astype(jnp.float32) + from_right.astype(jnp.float32)


def on_device(
    queries,
    draft_kv,
    kv_pool,
    block_dest,
    block_table,
    context_len,
    draft_len,
    accept_mask,
    out_weight,
    residual,
    norm_gain,
):
    rank_count = lax.axis_size("dp")
    pool_count = kv_pool.shape[0]
    capacity = 2 * pool_count // rank_count
    requests, heads_local, window, head_dim = queries.shape
    block_len = kv_pool.shape[3]
    pool = kv_pool.reshape(pool_count, 2 * block_len, head_dim)
    queries = queries.reshape(requests, heads_local * window, head_dim)
    drafts = draft_kv.reshape(requests, 2 * window, head_dim)
    kept_count = jnp.sum(jnp.cumprod(accept_mask, axis=1, dtype=jnp.int32), axis=1, dtype=jnp.int32)
    visible = context_len - window + kept_count

    rank = lax.axis_index("dp")
    rank_y, rank_z = over(rank, ring_len), rest(rank, ring_len)
    y_len = rank_count // ring_len
    ahead_y = rest(over(block_dest, ring_len) - rank_y, y_len)
    ahead_z = rest(block_dest - rank_z, ring_len)
    ahead = jnp.where(block_dest >= 0, ahead_y * ring_len + ahead_z, rank_count)
    steps = jnp.arange(rank_count, dtype=jnp.int32)
    counts = jnp.sum((ahead[None, :] == steps[:, None]).astype(jnp.int32), axis=1, dtype=jnp.int32)
    starts, _ = ring_starts(counts.reshape(y_len, ring_len))
    fixed = jnp.array([[0, 3, 6, 8], [1, 4, 7, 9], [2, 5, 11, 10]], jnp.int32) * capacity
    near_slots = 12 * capacity
    tables = by_distance(
        [fixed[n : n + 1] for n in range(3)],
        near_slots + starts[0],
        near_slots + room[0] + starts[1],
        0,
    )
    start = jnp.stack([table.T for table in tables], axis=-1).reshape(-1)
    outputs = pack_blocks(
        ahead,
        jnp.concatenate([start, jnp.zeros((2,), jnp.int32)]),
        pool,
        (3 * capacity, 5 * capacity, 4 * capacity, room[0], room[0]),
        lambda d: (d & (ring_len - 1)) == ring_len // 2,
    )
    along = neighbours(ring_len, y_len)
    carried = first_moves(outputs, along, capacity)

    all_counts = from_everyone(counts, "dp").reshape(rank_count, y_len, ring_len)
    all_starts, travelling = ring_starts(all_counts)
    limits = jnp.array(room[:0:-1], jnp.int32)
    fits = jnp.all(travelling <= limits)
    lengths = jnp.array([capacity // 2, capacity, capacity], jnp.int32)
    clamped = jnp.minimum(all_starts, (limits - lengths)[:, None])
    first = jnp.arange(24, dtype=jnp.int32).reshape(3, 2, 4)
    base = jnp.where(first >= 16, 28 * capacity + (first - 16) * (capacity // 2), (12 + first) * capacity)
    base = base[::-1].transpose(1, 0, 2) + all_starts - clamped
    by_r = jnp.arange(y_len, dtype=jnp.int32) * capacity
    near = [
        jnp.broadcast_to(n * y_len * capacity + by_r, (rank_count, 1, y_len)) for n in range(3)
    ]
    even, odd = by_distance(near, base[:, 0], base[:, 1], 1)
    source = jnp.arange(rank_count, dtype=jnp.int32)
    gap_y = rest(rank_y - over(source, ring_len), y_len)
    gap_z = rest(rank_z - source, ring_len)
    here = (gap_z[:, None, None] == jnp.arange(ring_len)[None, :, None]) & (
        gap_y[:, None, None] == jnp.arange(y_len)[None, None, :]
    )
    even = jnp.sum(jnp.where(here, even, 0), axis=(1, 2))
    odd = jnp.sum(jnp.where(here, odd, 0), axis=(1, 2))
    halved = gap_z == ring_len // 2
    steps_z = jnp.arange(2, 5, dtype=jnp.int32)[:, None] * jnp.array([1, -1], jnp.int32)[None]
    origin = rank_y * ring_len + rest(rank_z - steps_z, ring_len)
    chosen = (origin[:, :, None] == source[None, None, :]).astype(jnp.int32)
    by_step = clamped[:, :, ::-1].transpose(2, 1, 0, 3)
    offsets = jnp.sum(by_step * chosen[..., None], axis=2).reshape(-1)
    origin = over(block_table, capacity)
    order = rest(block_table, capacity)
    named = origin[:, :, None] == source[None, None, :]
    pick_from = lambda values: jnp.sum(jnp.where(named, values, 0), axis=2)
    table = jnp.where(rest(order, 2) == 0, pick_from(even), pick_from(odd))
    table = table + jnp.where(pick_from(halved.astype(jnp.int32)) > 0, over(order, 2), order)
    table, offsets, visible, fits = lax.optimization_barrier((table.reshape(-1), offsets, visible, fits))

    def by_rings(*carried):
        arrays, plan = along_rings(carried, offsets, along, capacity, room)
        return attend(table, visible, offsets, queries, drafts, arrays, plan, window)

    def by_exchange(*carried):
        start = jnp.repeat(jnp.arange(rank_count + 1, dtype=jnp.int32) * capacity, 2)
        dest = jnp.where(block_dest >= 0, block_dest, rank_count)
        slots = rank_count * capacity
        (packed,) = pack_blocks(dest, start, pool, (slots,), lambda d: d < 0)
        arrived = lax.all_to_all(packed, "dp", split_axis=0, concat_axis=0, tiled=True)
        piece = slots // load_pieces
        plan = [(0, ("at", p * piece), piece) for p in range(load_pieces)]
        no_offsets = jnp.zeros((1,), jnp.int32)
        return attend(block_table.reshape(-1), visible, no_offsets, queries, drafts, [arrived], plan, window, 1)

    token_rows = lax.cond(fits, by_rings, by_exchange, *carried)
    column_count = norm_gain.shape[0]
    place = lax.axis_index("mp")
    live_rows = (jnp.arange(window, dtype=jnp.int32)[None, :] < draft_len[:, None]).reshape(
        requests * window
    )
    share = project(token_rows, out_weight, column_count)
    local_residual = lax.dynamic_slice_in_dim(residual, place * column_count, column_count, 1)
    local_hidden = local_residual.astype(jnp.float32) + share
    squares = over_copies(jnp.sum(local_hidden * local_hidden, axis=1), "mp")
    mean_square = (squares / (column_count * lax.axis_size("mp")))[:, None]
    normed = local_hidden * lax.rsqrt(mean_square + norm_epsilon) * norm_gain[None, :]
    return jnp.where(live_rows[:, None], normed, 0.0).astype(jnp.bfloat16)


def solution(mesh):
    return jax.shard_map(
        on_device,
        mesh=mesh,
        in_specs=(
            P("dp", "mp", None, None),
            P("dp", None, "mp", None, None),
            P("dp", None, "mp", None, None),
            P("dp"),
            P("dp", None),
            P("dp"),
            P("dp"),
            P("dp", None),
            P("mp", None),
            P("dp", None),
            P("mp"),
        ),
        out_specs=P("dp", "mp"),
        check_vma=False,
    )
```

```python
import functools
import math

import jax
import jax.numpy as jnp
import numpy as np
from jax import lax
from jax.experimental import pallas as pl
from jax.experimental.pallas import tpu as pltpu
from jax.sharding import PartitionSpec as P


masked_score = -1e30
norm_epsilon = 1e-05
load_pieces = 2
ring_len = 8
room = (168, 168, 124, 52)


def over(array, power):
    return lax.shift_right_arithmetic(array, jnp.int32(power.bit_length() - 1))


def rest(array, power):
    return jnp.bitwise_and(array, power - 1)


def from_everyone(array, axis):
    length = lax.axis_size(axis)
    return lax.all_to_all(
        jnp.broadcast_to(array[None], (length, *array.shape)), axis, 0, 0, tiled=True
    )


def over_copies(array, axis):
    everything = from_everyone(array, axis)
    return jnp.sum(everything, axis=0)


def pack_kernel(halved, kinds, dest_ref, start_ref, pool_ref, *refs):
    outs, (staged, used, sem, out_sem) = refs[:-4], refs[-4:]
    blocks = pool_ref.shape[0]
    slots = staged.shape[0] - blocks

    def clear(d, carry):
        used[d] = 0
        return carry

    lax.fori_loop(0, kinds + 1, clear, 0)

    def place(b, carry):
        d = dest_ref[b]
        k = used[d]
        used[d] = k + 1
        slot = start_ref[2 * d + (k & 1)] + jnp.where(halved(d), k >> 1, k)
        slot = jnp.where(d < kinds, jnp.minimum(slot, slots - 1), slots + b)
        pltpu.make_async_copy(pool_ref.at[b], staged.at[slot], sem).start()
        return carry

    lax.fori_loop(0, blocks, place, 0, unroll=4 if len(outs) > 1 else 1)
    pltpu.make_async_copy(pool_ref, staged.at[pl.ds(0, blocks)], sem).wait()
    copies, at = [], 0
    for n, out in enumerate(outs):
        rows = pl.ds(at, out.shape[0])
        copies.append(pltpu.make_async_copy(staged.at[rows], out, out_sem.at[n]))
        at += out.shape[0]
    for copy in copies:
        copy.start()
    for copy in copies:
        copy.wait()


def pack_blocks(dest, start, pool, sizes, halved):
    kinds = start.shape[0] // 2 - 1
    return pl.pallas_call(
        functools.partial(pack_kernel, halved, kinds),
        out_shape=[jax.ShapeDtypeStruct((n,) + pool.shape[1:], pool.dtype) for n in sizes],
        in_specs=[
            pl.BlockSpec(memory_space=pltpu.SMEM),
            pl.BlockSpec(memory_space=pltpu.SMEM),
            pl.BlockSpec(memory_space=pl.ANY),
        ],
        out_specs=[pl.BlockSpec(memory_space=pl.ANY)] * len(sizes),
        scratch_shapes=[
            pltpu.VMEM((sum(sizes) + pool.shape[0],) + pool.shape[1:], pool.dtype),
            pltpu.SMEM((kinds + 1,), jnp.int32),
            pltpu.SemaphoreType.DMA,
            pltpu.SemaphoreType.DMA((len(sizes),)),
        ],
        cost_estimate=pl.CostEstimate(flops=1 << 28, bytes_accessed=1 << 23, transcendentals=0),
        name="pack_blocks",
    )(dest, start, pool)


def pick_kernel(plans, offset_ref, *refs):
    sources, outs, sem = refs[: -len(plans) - 1], refs[-len(plans) - 1 : -1], refs[-1]
    copies = []
    for plan, out in zip(plans, outs):
        at = 0
        for source, (kind, number), length in plan:
            start = offset_ref[number] if kind == "offset" else number
            copies.append(
                pltpu.make_async_copy(
                    sources[source].at[pl.ds(start, length)],
                    out.at[pl.ds(at, length)],
                    sem.at[len(copies)],
                )
            )
            at += length
    for copy in copies:
        copy.start()
    for copy in copies:
        copy.wait()


def pick(offsets, sources, plans):
    shape = sources[0].shape[1:]
    sizes = [sum(length for _, _, length in plan) for plan in plans]
    return pl.pallas_call(
        functools.partial(pick_kernel, plans),
        out_shape=[jax.ShapeDtypeStruct((n,) + shape, sources[0].dtype) for n in sizes],
        in_specs=[pl.BlockSpec(memory_space=pltpu.SMEM)]
        + [pl.BlockSpec(memory_space=pl.ANY)] * len(sources),
        out_specs=[pl.BlockSpec(memory_space=pltpu.VMEM)] * len(plans),
        scratch_shapes=[pltpu.SemaphoreType.DMA((sum(len(plan) for plan in plans),))],
        cost_estimate=pl.CostEstimate(flops=1 << 20, bytes_accessed=4 << 20, transcendentals=0),
        name="pick",
    )(offsets, *sources)


def attend_kernel(per_step, plan, table_ref, visible_ref, offset_ref, queries_ref, draft_ref, *refs):
    sources, (out_ref, cache, load_sem) = refs[:-3], refs[-3:]
    slots = cache.shape[0] - 1
    step = pl.program_id(0)
    width = table_ref.shape[0] // visible_ref.shape[0]
    block_len = cache.shape[1] // 2
    rows, head_dim = queries_ref.shape[1:]
    window = out_ref.shape[0] // per_step
    log_scale = math.log2(math.e) / math.sqrt(head_dim)

    @pl.when(step == 0)
    def _():
        copies, at = [], 0
        for source, (kind, number), length in plan:
            start = offset_ref[number] if kind == "offset" else number
            copies.append(
                pltpu.make_async_copy(
                    sources[source].at[pl.ds(start, length)],
                    cache.at[pl.ds(at, length)],
                    load_sem.at[len(copies)],
                )
            )
            at += length
        for copy in copies:
            copy.start()
        cache[slots] = jnp.zeros_like(cache[slots])
        for copy in copies:
            copy.wait()

    positions = lax.broadcasted_iota(jnp.int32, (rows, width * block_len), 1)
    query_place = rest(lax.broadcasted_iota(jnp.int32, (rows, window), 0), window)
    causal = lax.broadcasted_iota(jnp.int32, (rows, window), 1) <= query_place
    over_last = (((1,), (1,)), ((), ()))
    for n in range(per_step):
        request = step * per_step + n
        visible = visible_ref[request]
        places = [
            jnp.where(e * block_len < visible, table_ref[request * width + e], slots)
            for e in range(width)
        ]
        keys = jnp.concatenate([cache[s, :block_len, :] for s in places], axis=0)
        values = jnp.concatenate([cache[s, block_len:, :] for s in places], axis=0)
        query = queries_ref[n]
        cached = lax.dot_general(query, keys, over_last, preferred_element_type=jnp.float32)
        cached = jnp.where(positions < visible, cached, masked_score)
        drafts = lax.dot_general(
            query, draft_ref[n, :window, :], over_last, preferred_element_type=jnp.float32
        )
        drafts = jnp.where(causal, drafts, masked_score)
        row_max = jnp.maximum(
            jnp.max(cached, axis=1, keepdims=True), jnp.max(drafts, axis=1, keepdims=True)
        )
        cached = jnp.exp2((cached - row_max) * log_scale)
        drafts = jnp.exp2((drafts - row_max) * log_scale)
        denominator = jnp.sum(cached, axis=1, keepdims=True) + jnp.sum(drafts, axis=1, keepdims=True)
        attended = jnp.dot(cached.astype(jnp.bfloat16), values, preferred_element_type=jnp.float32)
        attended = attended + jnp.dot(
            drafts.astype(jnp.bfloat16), draft_ref[n, window:, :], preferred_element_type=jnp.float32
        )
        attended = (attended / denominator).astype(jnp.bfloat16)
        for h in range(rows // window):
            out_ref[n * window : (n + 1) * window, h * head_dim : (h + 1) * head_dim] = attended[
                h * window : (h + 1) * window
            ]


def attend(table, visible, offsets, queries, drafts, sources, plan, window, per_step=4):
    requests, rows, head_dim = queries.shape
    slots = sum(length for _, _, length in plan)
    return pl.pallas_call(
        functools.partial(attend_kernel, per_step, plan),
        out_shape=jax.ShapeDtypeStruct((requests * window, rows // window * head_dim), jnp.bfloat16),
        grid_spec=pltpu.PrefetchScalarGridSpec(
            num_scalar_prefetch=3,
            grid=(requests // per_step,),
            in_specs=[
                pl.BlockSpec((per_step, rows, head_dim), lambda i, *_: (i, 0, 0)),
                pl.BlockSpec((per_step,) + drafts.shape[1:], lambda i, *_: (i, 0, 0)),
            ]
            + [pl.BlockSpec(memory_space=pl.ANY)] * len(sources),
            out_specs=pl.BlockSpec(
                (per_step * window, rows // window * head_dim), lambda i, *_: (i, 0)
            ),
            scratch_shapes=[
                pltpu.VMEM((slots + 1,) + sources[0].shape[1:], sources[0].dtype),
                pltpu.SemaphoreType.DMA((len(plan),)),
            ],
        ),
        cost_estimate=pl.CostEstimate(flops=1 << 30, bytes_accessed=10 << 20, transcendentals=1 << 21),
        name="attend",
    )(table, visible, offsets, queries, drafts, *sources)


def ring_starts(counts):
    middle = counts[..., 4]
    up = jnp.stack([over(middle + 1, 2), counts[..., 3], counts[..., 2]], axis=-2)
    down = jnp.stack([over(middle, 2), counts[..., 5], counts[..., 6]], axis=-2)
    both = jnp.stack([up, down], axis=-3)
    flat = both.reshape(both.shape[:-2] + (12,))
    before = (jnp.arange(12)[:, None] < jnp.arange(12)[None, :]).astype(jnp.int32)
    starts = jnp.sum(flat[..., :, None] * before, axis=-2).reshape(both.shape)
    group = both.sum(axis=-1)
    upto = (jnp.arange(3)[:, None] <= jnp.arange(3)[None, :]).astype(jnp.int32)
    travelling = jnp.sum(group[..., :, None] * upto, axis=-2)
    return starts, travelling


def pack_table(capacity, y_len, ring_len, first_room):
    fixed = {0: (0, 3, 6, 8), 1: (1, 4, 7, 9), ring_len - 1: (2, 5, 11, 10)}
    kinds = y_len * ring_len
    base = np.zeros((2 * kinds + 2,), np.int32)
    weights = np.zeros((2 * kinds + 2, 3, kinds), np.int32)
    for way, order in enumerate(((4, 3, 2), (4, 5, 6))):
        earlier = []
        for q in order:
            for r in range(y_len):
                d = r * ring_len + q
                for parity in (way,) if q == 4 else (0, 1):
                    base[2 * d + parity] = 12 * capacity + way * first_room
                    for part, e in earlier:
                        weights[2 * d + parity, part, e] = 1
                earlier.append((1 + way if q == 4 else 0, d))
    for q, places in fixed.items():
        for r, place in enumerate(places):
            d = r * ring_len + q
            base[2 * d : 2 * d + 2] = place * capacity
    return jnp.asarray(base), jnp.asarray(weights)


def by_distance(near, up, down, axis):
    part = lambda array, g: lax.slice_in_dim(array, g, g + 1, axis=axis)
    tables = []
    for middle in (up, down):
        parts = [near[0], near[1], part(up, 2), part(up, 1), part(middle, 0), part(down, 1), part(down, 2), near[2]]
        tables.append(jnp.concatenate(parts, axis=axis))
    return tables


def neighbours(ring_len, y_len):
    size = y_len * ring_len
    return (
        [(i, i // ring_len * ring_len + (i + 1) % ring_len) for i in range(size)],
        [(i, i // ring_len * ring_len + (i - 1) % ring_len) for i in range(size)],
        [(i, (i + ring_len) % size) for i in range(size)],
        [(i, (i - ring_len) % size) for i in range(size)],
    )


def first_moves(outputs, along, full):
    own, for_forth, for_back, rising, falling = outputs
    up, down, forth, back = along
    for _ in range(1, 3):
        rising = lax.ppermute(rising, "dp", up)
        falling = lax.ppermute(falling, "dp", down)
    forth_0 = lax.ppermute(for_forth, "dp", forth)
    back_0 = lax.ppermute(for_back, "dp", back)
    forth_00 = lax.ppermute(lax.slice_in_dim(forth_0, 3 * full, 5 * full), "dp", forth)
    back_00 = lax.ppermute(lax.slice_in_dim(back_0, 3 * full, 4 * full), "dp", back)
    return own, forth_0, back_0, forth_00, back_00, rising, falling


def along_rings(carried, offsets, along, capacity, room):
    own, forth_0, back_0, forth_00, back_00, rising, falling = carried
    up, down, forth, back = along
    full, half = capacity, capacity // 2
    arrays = [own, forth_0, back_0, forth_00, back_00]
    home = [(0, ("at", 0), full), (1, ("at", 0), full), (3, ("at", 0), full), (2, ("at", 0), full)]
    for_up = [(0, ("at", full), full), (1, ("at", full), full), (3, ("at", full), full), (2, ("at", full), full)]
    for_down = [(0, ("at", 2 * full), full), (1, ("at", 2 * full), full), (4, ("at", 0), full), (2, ("at", 2 * full), full)]
    found = {}

    def keep(array):
        arrays.append(array)
        return len(arrays) - 1

    passing_forth = passing_back = None
    for t in range(2, 5):
        u, d = keep(rising), keep(falling)
        if t < 4:
            rising = lax.ppermute(lax.slice_in_dim(rising, 0, room[t]), "dp", up)
            falling = lax.ppermute(lax.slice_in_dim(falling, 0, room[t]), "dp", down)
        length = full if t < 4 else half

        def piece(direction, r):
            number = ((t - 2) * 2 + direction) * 4 + r
            return ((u, d)[direction], ("offset", number), length)

        found[0, t, 0], found[1, t, 0] = piece(0, 0), piece(1, 0)
        forward = [piece(0, 1), piece(1, 1)]
        backward = [piece(0, 3), piece(1, 3)]
        plans = [forward, backward]
        if t < 4:
            forward.append(piece(0, 2))
            backward.append(piece(1, 2))
        else:
            plans.append([piece(0, 2), piece(1, 2)])
        passed_at = sum(n for _, _, n in forward)
        for plan, passing in ((forward, passing_forth), (backward, passing_back)):
            if passing is not None:
                plan.append((passing[0], ("at", passing[1]), passing[2]))
        needed = sorted({p[0] for plan in plans for p in plan})
        renamed = [
            [(needed.index(source), start, n) for source, start, n in plan] for plan in plans
        ]
        send_forth, send_back, *across = pick(offsets, [arrays[i] for i in needed], renamed)
        f = keep(lax.ppermute(send_forth, "dp", forth))
        b = keep(lax.ppermute(send_back, "dp", back))
        found[0, t, 1], found[1, t, 1] = (f, ("at", 0), length), (f, ("at", length), length)
        found[0, t, 3], found[1, t, 3] = (b, ("at", 0), length), (b, ("at", length), length)
        if t > 2:
            found[0, t - 1, 2] = (f, ("at", passed_at), full)
            found[1, t - 1, 2] = (b, ("at", passed_at), full)
        passing_forth, passing_back = (f, 2 * length, length), (b, 2 * length, length)
    near_up, near_down = pick(offsets, arrays[:5], [for_up, for_down])
    near_up = keep(lax.ppermute(near_up, "dp", up))
    near_down = keep(lax.ppermute(near_down, "dp", down))
    two_on = [(start, forth[middle][1]) for start, middle in forth]
    last = keep(lax.ppermute(across[0], "dp", two_on))
    found[0, 4, 2], found[1, 4, 2] = (last, ("at", 0), half), (last, ("at", half), half)
    plan = home + [(near_up, ("at", 0), 4 * full), (near_down, ("at", 0), 4 * full)]
    plan += [found[direction, t, r] for t in range(2, 5) for direction in range(2) for r in range(4)]
    return arrays, plan


def project(token_rows, out_weight, column_count):
    size = lax.axis_size("mp")
    chips = size // 2
    place = lax.axis_index("mp")
    core = rest(place, 2)
    swap = [(i, i ^ 1) for i in range(size)]
    right = [(i, (i + 2) % size) for i in range(size)]
    left = [(i, (i - 2) % size) for i in range(size)]

    def columns(k, c):
        chip = rest(over(place, 2) + k, chips)
        return lax.dynamic_slice_in_dim(out_weight, (chip * 2 + c) * column_count, column_count, 1)

    own_weight = [columns(k, core) for k in range(chips)]
    given = jnp.concatenate([columns(k, 1 - core) for k in range(chips)], axis=0)
    their_weight = jnp.split(lax.ppermute(given, "mp", swap), chips, axis=0)
    theirs = lax.ppermute(token_rows, "mp", swap)

    def own_part(k):
        own = jnp.dot(token_rows, own_weight[k], preferred_element_type=jnp.float32)
        return lax.optimization_barrier(own)

    own_far = own_part(2)
    own_ahead = own_part(1)

    def with_theirs(own, k):
        return own + jnp.dot(theirs, their_weight[k], preferred_element_type=jnp.float32)

    half = column_count // 2
    far = with_theirs(own_far, 2).astype(jnp.bfloat16)
    from_left = lax.ppermute(far[:, :half], "mp", right)
    from_right = lax.ppermute(far[:, half:], "mp", left)
    ahead = with_theirs(own_ahead, 1)
    behind = with_theirs(own_part(3), 3)
    home = with_theirs(own_part(0), 0)
    ahead = jnp.concatenate([ahead[:, :half] + from_left.astype(jnp.float32), ahead[:, half:]], axis=1)
    behind = jnp.concatenate([behind[:, :half], behind[:, half:] + from_right.astype(jnp.float32)], axis=1)
    from_left = lax.ppermute(ahead.astype(jnp.bfloat16), "mp", right)
    from_right = lax.ppermute(behind.astype(jnp.bfloat16), "mp", left)
    return home + from_left.astype(jnp.float32) + from_right.astype(jnp.float32)


def on_device(
    queries,
    draft_kv,
    kv_pool,
    block_dest,
    block_table,
    context_len,
    draft_len,
    accept_mask,
    out_weight,
    residual,
    norm_gain,
):
    rank_count = lax.axis_size("dp")
    pool_count = kv_pool.shape[0]
    capacity = 2 * pool_count // rank_count
    requests, heads_local, window, head_dim = queries.shape
    block_len = kv_pool.shape[3]
    pool = kv_pool.reshape(pool_count, 2 * block_len, head_dim)
    queries = queries.reshape(requests, heads_local * window, head_dim)
    drafts = draft_kv.reshape(requests, 2 * window, head_dim)
    kept_count = jnp.sum(jnp.cumprod(accept_mask, axis=1, dtype=jnp.int32), axis=1, dtype=jnp.int32)
    visible = context_len - window + kept_count

    rank = lax.axis_index("dp")
    rank_y, rank_z = over(rank, ring_len), rest(rank, ring_len)
    y_len = rank_count // ring_len
    ahead_y = rest(over(block_dest, ring_len) - rank_y, y_len)
    ahead_z = rest(block_dest - rank_z, ring_len)
    ahead = jnp.where(block_dest >= 0, ahead_y * ring_len + ahead_z, rank_count)
    steps = jnp.arange(rank_count, dtype=jnp.int32)
    counts = jnp.sum((ahead[None, :] == steps[:, None]).astype(jnp.int32), axis=1, dtype=jnp.int32)
    base, weights = pack_table(capacity, y_len, ring_len, room[0])
    parts = jnp.stack([counts, over(counts + 1, 2), over(counts, 2)])
    start = base + jnp.sum(weights * parts[None], axis=(1, 2), dtype=jnp.int32)
    outputs = pack_blocks(
        ahead,
        start,
        pool,
        (3 * capacity, 5 * capacity, 4 * capacity, room[0], room[0]),
        lambda d: (d & (ring_len - 1)) == ring_len // 2,
    )
    along = neighbours(ring_len, y_len)
    carried = first_moves(outputs, along, capacity)

    all_counts = from_everyone(counts, "dp").reshape(rank_count, y_len, ring_len)
    all_starts, travelling = ring_starts(all_counts)
    limits = jnp.array(room[:0:-1], jnp.int32)
    fits = jnp.all(travelling <= limits)
    lengths = jnp.array([capacity // 2, capacity, capacity], jnp.int32)
    clamped = jnp.minimum(all_starts, (limits - lengths)[:, None])
    first = jnp.arange(24, dtype=jnp.int32).reshape(3, 2, 4)
    base = jnp.where(first >= 16, 28 * capacity + (first - 16) * (capacity // 2), (12 + first) * capacity)
    base = base[::-1].transpose(1, 0, 2) + all_starts - clamped
    by_r = jnp.arange(y_len, dtype=jnp.int32) * capacity
    near = [
        jnp.broadcast_to(n * y_len * capacity + by_r, (rank_count, 1, y_len)) for n in range(3)
    ]
    even, odd = by_distance(near, base[:, 0], base[:, 1], 1)
    source = jnp.arange(rank_count, dtype=jnp.int32)
    gap_y = rest(rank_y - over(source, ring_len), y_len)
    gap_z = rest(rank_z - source, ring_len)
    here = (gap_z[:, None, None] == jnp.arange(ring_len)[None, :, None]) & (
        gap_y[:, None, None] == jnp.arange(y_len)[None, None, :]
    )
    even = jnp.sum(jnp.where(here, even, 0), axis=(1, 2))
    odd = jnp.sum(jnp.where(here, odd, 0), axis=(1, 2))
    halved = gap_z == ring_len // 2
    steps_z = jnp.arange(2, 5, dtype=jnp.int32)[:, None] * jnp.array([1, -1], jnp.int32)[None]
    origin = rank_y * ring_len + rest(rank_z - steps_z, ring_len)
    chosen = (origin[:, :, None] == source[None, None, :]).astype(jnp.int32)
    by_step = clamped[:, :, ::-1].transpose(2, 1, 0, 3)
    offsets = jnp.sum(by_step * chosen[..., None], axis=2).reshape(-1)
    origin = over(block_table, capacity)
    order = rest(block_table, capacity)
    named = origin[:, :, None] == source[None, None, :]
    pick_from = lambda values: jnp.sum(jnp.where(named, values, 0), axis=2)
    table = jnp.where(rest(order, 2) == 0, pick_from(even), pick_from(odd))
    table = table + jnp.where(pick_from(halved.astype(jnp.int32)) > 0, over(order, 2), order)
    table, offsets, visible, fits = lax.optimization_barrier((table.reshape(-1), offsets, visible, fits))

    def by_rings(*carried):
        arrays, plan = along_rings(carried, offsets, along, capacity, room)
        return attend(table, visible, offsets, queries, drafts, arrays, plan, window)

    def by_exchange(*carried):
        start = jnp.repeat(jnp.arange(rank_count + 1, dtype=jnp.int32) * capacity, 2)
        dest = jnp.where(block_dest >= 0, block_dest, rank_count)
        slots = rank_count * capacity
        (packed,) = pack_blocks(dest, start, pool, (slots,), lambda d: d < 0)
        arrived = lax.all_to_all(packed, "dp", split_axis=0, concat_axis=0, tiled=True)
        piece = slots // load_pieces
        plan = [(0, ("at", p * piece), piece) for p in range(load_pieces)]
        no_offsets = jnp.zeros((1,), jnp.int32)
        return attend(block_table.reshape(-1), visible, no_offsets, queries, drafts, [arrived], plan, window, 1)

    token_rows = lax.cond(fits, by_rings, by_exchange, *carried)
    column_count = norm_gain.shape[0]
    place = lax.axis_index("mp")
    live_rows = (jnp.arange(window, dtype=jnp.int32)[None, :] < draft_len[:, None]).reshape(
        requests * window
    )
    share = project(token_rows, out_weight, column_count)
    local_residual = lax.dynamic_slice_in_dim(residual, place * column_count, column_count, 1)
    local_hidden = local_residual.astype(jnp.float32) + share
    squares = over_copies(jnp.sum(local_hidden * local_hidden, axis=1), "mp")
    mean_square = (squares / (column_count * lax.axis_size("mp")))[:, None]
    normed = local_hidden * lax.rsqrt(mean_square + norm_epsilon) * norm_gain[None, :]
    return jnp.where(live_rows[:, None], normed, 0.0).astype(jnp.bfloat16)


def solution(mesh):
    return jax.shard_map(
        on_device,
        mesh=mesh,
        in_specs=(
            P("dp", "mp", None, None),
            P("dp", None, "mp", None, None),
            P("dp", None, "mp", None, None),
            P("dp"),
            P("dp", None),
            P("dp"),
            P("dp"),
            P("dp", None),
            P("mp", None),
            P("dp", None),
            P("mp"),
        ),
        out_specs=P("dp", "mp"),
        check_vma=False,
    )
```
